512 devices in a mesh: ep: 128 (over x, z, core), dp: 4 (over y).
Axes of the slice: x: 4, y: 4, z: 16, core: 2. Of those that a mesh axis runs over, the one named last changes fastest.
Arguments:
- tokens: bfloat16 [2048, 3584], P('ep'), may hold values from -6 to 6
- expert_ids: int32 [2048, 8], P('ep'), may hold values from 0 to 127, all different within a row; in each aligned block of 16 rows (0 to 15, 16 to 31, ...) at most 4 rows name the same one
- route_logits: float32 [2048, 8], P('ep'), may hold values from -8 to 8
- expert_gate: bfloat16 [128, 3584, 1024], P('ep', None, 'dp'), may hold values from -0.09375 to 0.09375
- expert_up: bfloat16 [128, 3584, 1024], P('ep', None, 'dp'), may hold values from -0.09375 to 0.09375
- expert_down: bfloat16 [128, 1024, 3584], P('ep', 'dp'), may hold values from -0.1875 to 0.1875
Outputs:
- mixed: bfloat16 [2048, 3584], P(('ep', 'dp'))
The draws below stay inside these ranges and needn't reach their ends.
Inputs may be any that keep to these rules, and one draw needn't show every extreme that they name: `expert_ids`: each row names 8 different experts of 0 to 127 and every expert is named by some row. Within the rows of one index of ep (aligned blocks of 16 rows) no expert is named more than 4 times, and some block names one expert exactly 4 times. Loads are heavy-tailed: a few experts take several times the mean.
All inputs are finite; a program needn't handle non-finite values.
Results may differ from the reference program's by a relative error of at most 0.015.
Values may be sent and summed in bfloat16 or wider, within the bound.
A program may use at most 64 MiB of HBM per device.

```python
import math
import jax
import jax.numpy as jnp
import numpy as np
from jax import lax

D = 3584
FF = 1024
TOP = 8
TOK_EP = 16
EXPERTS = 128
TOKENS = 2048
CAP = 4


def block_levels(own_key, shape, cuts, smallest, largest):
    gain = 1.0
    for position, parts in cuts:
        steps = jax.random.uniform(jax.random.fold_in(jax.random.fold_in(own_key, 6), position), (parts,), jnp.float32, smallest / len(cuts), largest / len(cuts))
        gain = gain * jnp.repeat(jnp.exp(steps), shape[position] // parts).reshape((-1,) + (1,) * (len(shape) - 1 - position))
    return gain


def deal_out(key, own, number, rows, amount, top, reach, lean):
    sequence = jax.random.permutation(key, amount)
    heavy_load, usual = load_shares(amount, rows * top, reach, lean, True), load_shares(amount, rows * top, reach, lean, False)
    places = jnp.arange(amount)

    def named(tallies, rotation):
        used = int((tallies > 0).sum())
        fixed = max(1, used // 4)
        shifted = fixed + (places - fixed + rotation * (used - fixed)) % max(1, amount - fixed)
        return jnp.zeros((amount,), jnp.int32).at[sequence[jnp.where(places < fixed, places, shifted)]].set(jnp.asarray(tallies, jnp.int32))

    tallies = jnp.where(number % 4 == 0, named(heavy_load, number // 4), named(usual, number - number // 4 - 1))
    mixed = jax.random.permutation(jax.random.fold_in(own, 3), amount)
    donor, taker = mixed[0:amount // 2 * 2:2], mixed[1:amount // 2 * 2:2]
    margin = jnp.minimum(tallies[donor] - 1, reach - tallies[taker]) // 2
    margin = jnp.where((donor == sequence[0]) | (taker == sequence[0]) | (tallies[taker] == 0), 0, jnp.maximum(margin, 0))
    shifted = jax.random.randint(jax.random.fold_in(own, 4), (amount // 2,), 0, 1 << 20) % (margin + 1)
    tallies = tallies.at[donor].add(-shifted).at[taker].add(shifted)
    members = jnp.searchsorted(jnp.cumsum(tallies), jnp.arange(rows * top), side="right").astype(jnp.int32)
    listing = members.reshape(top, rows).T
    listing = listing[jax.random.permutation(jax.random.fold_in(own, 1), rows)]
    rotation = jax.random.randint(jax.random.fold_in(own, 2), (rows, 1), 0, top)
    return jnp.take_along_axis(listing, (jnp.arange(top)[None, :] + rotation) % top, axis=1)


def load_shares(count, total, bound, slope, full):
    loads = [(1 << 20) // math.isqrt(standing ** slope) + 1 for standing in range(1, count + 1)]
    largest = bound if full else min(bound, max(-(-total // count), total * loads[0] // sum(loads)))
    least = 1 if total - largest >= count - 1 else 0
    given, spare = [largest] + [least] * (count - 1), total - largest - least * (count - 1)
    while spare > 0:
        free = [i for i in range(1, count) if given[i] < largest] or [i for i in range(1, count) if given[i] < bound]
        pool, remaining = sum([loads[i] for i in free]), spare
        for i in free:
            extra = min(bound - given[i], max(1, remaining * loads[i] // pool), spare)
            given[i] = given[i] + extra
            spare = spare - extra
    return np.array(given)


def scatter_about(rng, extent, scale, most, cuts=(), held_as=jnp.bfloat16):
    result = jax.random.normal(rng, extent, jnp.float32) * scale
    if len(cuts) > 0:
        result = block_levels(rng, extent, cuts, -0.22, 0.18) * result
    return jnp.clip(result, min=-most, max=most).astype(held_as)


def setup_inputs(seed: int = 0) -> dict:
    key_of = jax.random.split(jax.random.key(seed), 7)
    tokens = scatter_about(key_of[0], (TOKENS, D), 1.0, 6.0, ((0, 128),))
    expert_ids_keys = jax.random.split(jax.random.fold_in(key_of[1], 1), TOKENS // TOK_EP)
    expert_ids_turns = jax.random.permutation(jax.random.fold_in(key_of[1], 3), TOKENS // TOK_EP)
    expert_ids = jax.vmap(lambda own, number: deal_out(jax.random.fold_in(key_of[1], 2), own, number, TOK_EP, EXPERTS, TOP, CAP, 3))(expert_ids_keys, expert_ids_turns).reshape((TOKENS, TOP))
    route_logits = scatter_about(key_of[2], (TOKENS, TOP), 2.0, 8.0, ((0, 128),), jnp.float32)
    expert_gate = scatter_about(key_of[3], (EXPERTS, D, FF), D ** -0.5, 0.09375, ((0, 128), (2, 4)))
    expert_up = scatter_about(key_of[4], (EXPERTS, D, FF), D ** -0.5, 0.09375, ((0, 128), (2, 4)))
    expert_down = scatter_about(key_of[5], (EXPERTS, FF, D), FF ** -0.5, 0.1875, ((0, 128), (1, 4)))
    return dict(tokens=tokens, expert_ids=expert_ids, route_logits=route_logits, expert_gate=expert_gate, expert_up=expert_up, expert_down=expert_down)


route_scale = 2.5


def expert_rows(rows, w_gate, w_up, w_down):
    gate = jnp.dot(rows, w_gate, preferred_element_type=jnp.float32)
    upper = jnp.dot(rows, w_up, preferred_element_type=jnp.float32)
    hidden = (jax.nn.silu(gate) * upper).astype(jnp.bfloat16)
    return jnp.dot(hidden, w_down, preferred_element_type=jnp.float32).astype(jnp.bfloat16)


def reference(tokens, expert_ids, route_logits, expert_gate, expert_up, expert_down):
    token_count, width = tokens.shape
    top = expert_ids.shape[1]
    experts = expert_gate.shape[0]
    flat_ids = expert_ids.reshape(-1).astype(jnp.int32)
    slots = flat_ids.shape[0]
    block_rows = 64
    counts = jnp.zeros((experts,), jnp.int32).at[flat_ids].add(1).astype(jnp.int32)
    padded = (((counts + block_rows - 1) // block_rows) * block_rows).astype(jnp.int32)
    pad_start = (jnp.cumsum(padded) - padded).astype(jnp.int32)
    seg_start = (jnp.cumsum(counts) - counts).astype(jnp.int32)
    sorted_slots = jnp.argsort(flat_ids, stable=True).astype(jnp.int32)
    sorted_ids = flat_ids[sorted_slots]
    within = (jnp.arange(slots, dtype=jnp.int32) - seg_start[sorted_ids]).astype(jnp.int32)
    target = (pad_start[sorted_ids] + within).astype(jnp.int32)
    nblocks = (slots + experts * (block_rows - 1)) // block_rows + 1
    row_token = jnp.full((nblocks * block_rows,), token_count, jnp.int32).at[target].set((sorted_slots // top).astype(jnp.int32))
    pad_end = pad_start + padded
    block_start = jnp.arange(nblocks, dtype=jnp.int32) * block_rows
    block_expert = jnp.sum((pad_end[None, :] <= block_start[:, None]).astype(jnp.int32), axis=1)
    block_expert = jnp.minimum(block_expert, experts - 1).astype(jnp.int32)
    extended = jnp.concatenate([tokens, jnp.zeros((1, width), tokens.dtype)], axis=0)

    def one_block(inputs):
        block_index, expert = inputs
        picks = lax.dynamic_slice_in_dim(row_token, (block_index * block_rows).astype(jnp.int32), block_rows, 0)
        return expert_rows(extended[picks], expert_gate[expert], expert_up[expert], expert_down[expert])

    outputs = lax.map(one_block, (jnp.arange(nblocks, dtype=jnp.int32), block_expert))
    outputs = outputs.reshape(nblocks * block_rows, width)
    slot_target = jnp.zeros((slots,), jnp.int32).at[sorted_slots].set(target)
    slot_values = outputs[slot_target].reshape(token_count, top, width)
    scores = jax.nn.sigmoid(route_logits)
    weights = route_scale * scores / jnp.sum(scores, axis=1, keepdims=True)
    routed = jnp.sum(weights[:, :, None] * slot_values.astype(jnp.float32), axis=1)
    return routed.astype(jnp.bfloat16)
```

```python
import functools

import jax
import jax.numpy as jnp
from jax import lax
from jax.experimental import pallas as pl
from jax.experimental.pallas import tpu as pltpu
from jax.sharding import PartitionSpec as P

route_scale = 2.5


def by_slots(tokens, expert_ids, route_logits, expert_gate, expert_up, expert_down):
    tok_rows, width = tokens.shape
    top = expert_ids.shape[1]
    n_ep = lax.axis_size("ep")
    n_dp = lax.axis_size("dp")
    experts = n_ep
    capacity = min(tok_rows, 4 * max(1, tok_rows * top // experts))
    flat_ids = expert_ids.reshape(-1).astype(jnp.int32)
    onehot = (flat_ids[:, None] == jnp.arange(experts, dtype=jnp.int32)[None, :]).astype(jnp.int32)
    earlier = jnp.cumsum(onehot, axis=0).astype(jnp.int32) - onehot
    within = jnp.sum(earlier * onehot, axis=1).astype(jnp.int32)
    slot_index = flat_ids * capacity + within
    token_of_slot = jnp.arange(tok_rows * top, dtype=jnp.int32) // top
    source_row = (
        jnp.full((experts * capacity,), tok_rows, jnp.int32).at[slot_index].set(token_of_slot)
    )
    extended = jnp.concatenate([tokens, jnp.zeros((1, width), tokens.dtype)], axis=0)
    outgoing = extended[source_row].reshape(n_ep, capacity, width)
    arrived = lax.all_to_all(outgoing, "ep", split_axis=0, concat_axis=0, tiled=True)
    received = arrived.reshape(n_ep * capacity, width)
    gate = jnp.dot(received, expert_gate[0], preferred_element_type=jnp.float32)
    upper = jnp.dot(received, expert_up[0], preferred_element_type=jnp.float32)
    hidden = (jax.nn.silu(gate) * upper).astype(jnp.bfloat16)
    partial_value = jnp.dot(hidden, expert_down[0], preferred_element_type=jnp.float32)
    partial_value = partial_value.reshape(n_ep, capacity, width)
    scores = jax.nn.sigmoid(route_logits)
    weights = route_scale * scores / jnp.sum(scores, axis=1, keepdims=True)
    member = lax.axis_index("dp")
    quarter = capacity // n_dp
    reduced = (
        lax.psum_scatter(partial_value.astype(jnp.bfloat16), "dp", scatter_dimension=1, tiled=True)
        .astype(jnp.float32)
        .astype(jnp.bfloat16)
    )
    back = lax.all_to_all(reduced, "ep", split_axis=0, concat_axis=0, tiled=True)
    offset = within - member * quarter
    held = ((offset >= 0) & (offset < quarter)).astype(jnp.float32)
    picked = flat_ids * quarter + jnp.clip(offset, 0, quarter - 1)
    values = back.reshape(experts * quarter, width)[picked].reshape(tok_rows, top, width)
    masked = weights * held.reshape(tok_rows, top)
    contrib = jnp.sum(masked[:, :, None] * values.astype(jnp.float32), axis=1)
    routed = lax.psum_scatter(
        contrib.astype(jnp.bfloat16), "dp", scatter_dimension=0, tiled=True
    ).astype(jnp.float32)
    return routed.astype(jnp.bfloat16)


MESH = pl.DeviceIdType.MESH
LANES = 128
SLOTS = 4


def exchange_kernel(
    nx, nz, per, tokens_ref, ids_ref, logits_ref, gate_hbm, up_hbm, down_hbm, out_ref,
    w_gate, w_up, w_down, block, lift, sent, gathered, own, other, from_y, summed, back,
    local, line_out, line_in, last_out, last_in,
    weight_sem, z_send, z_recv, x_send, x_recv, y_send, y_recv, ry_send, ry_recv,
    rx_send, rx_recv, rz_send, rz_recv, last_send, last_recv,
):
    rows, width = tokens_ref.shape
    top = ids_ref.shape[1]
    half, quarter = width // 2, width // 4
    reach = nz // 2
    groups = nz // per
    tall = per * SLOTS
    wide = 2 * nx * tall
    me, y = lax.axis_index("ep"), lax.axis_index("dp")
    c, z, x = me % 2, (me // 2) % nz, me // (2 * nz)
    mine = y % 2
    seat = 2 * x + c

    def device(i, d, h, j):
        xx, zz, yy = (x + i + nx) % nx, (z + d + nz) % nz, (y + j + 4) % 4
        return ((xx * nz + zz) * 2 + (c + h) % 2, yy)

    def remote(src, dst, send, recv, to):
        return pltpu.make_async_remote_copy(
            src_ref=src, dst_ref=dst, send_sem=send, recv_sem=recv,
            device_id=to, device_id_type=MESH,
        )

    loads = [
        pltpu.make_async_copy(src.at[0], dst, weight_sem.at[i])
        for i, (src, dst) in enumerate(((gate_hbm, w_gate), (up_hbm, w_up), (down_hbm, w_down)))
    ]
    for load in loads:
        load.start()

    others = [(i, h) for i in range(nx) for h in range(2) if i or h]
    peers = [device(0, 1, 0, 0), device(0, -1, 0, 0)]
    peers += [device(i, 0, h, 0) for i, h in others]
    peers += [device(0, 0, 0, j) for j in (1, 2, 3)]
    barrier = pltpu.get_barrier_semaphore()
    for peer in peers:
        pl.semaphore_signal(barrier, inc=1, device_id=peer, device_id_type=MESH)

    def lanes_of(part, size):
        return pl.ds(pl.multiple_of(part * size, LANES), size)

    scores = jax.nn.sigmoid(logits_ref[...])
    weights = route_scale * scores / jnp.sum(scores, axis=1, keepdims=True)
    lane = lax.broadcasted_iota(jnp.int32, (rows, LANES), 1)
    dense = jnp.zeros((rows, LANES), jnp.float32)
    for k in range(top):
        dense = dense + jnp.where(lane == ids_ref[:, k : k + 1], weights[:, k : k + 1], 0.0)
    block[z, :, :half] = tokens_ref[:, lanes_of(mine, half)]
    block[z, :, half:] = dense.astype(jnp.bfloat16)

    span = per * rows
    column = lax.broadcasted_iota(jnp.int32, (LANES, wide), 1) // tall
    expert = ((column // 2) * nz + z) * 2 + column % 2
    chosen_by = (lax.broadcasted_iota(jnp.int32, (LANES, wide), 0) == expert).astype(jnp.bfloat16)
    first = lax.broadcasted_iota(jnp.int32, (span, span), 0)
    second = lax.broadcasted_iota(jnp.int32, (span, span), 1)
    before = ((first // rows == second // rows) & (second < first)).astype(jnp.bfloat16)
    slot = lax.broadcasted_iota(jnp.int32, (span, wide), 1) % tall
    at_row = lax.broadcasted_iota(jnp.int32, (span, wide), 0)
    in_block = slot // SLOTS == at_row // rows
    slot_rank = (slot % SLOTS).astype(jnp.float32)

    pl.semaphore_wait(barrier, len(peers))

    def z_copy(way, d):
        at = (z - d + 1 + nz) % nz if way == 0 else (z + d - 1) % nz
        to = device(0, 1 if way == 0 else -1, 0, 0)
        return remote(block.at[at], block.at[at], z_send.at[way, d], z_recv.at[way, d], to)

    def place(order):
        step = (order + 1) // 2
        return (jnp.where(order % 2 == 1, z - step, z + step) + nz) % nz

    def x_copy(k, i, h):
        to = 2 * ((x + i) % nx) + (c + h) % 2
        return remote(
            sent.at[k, to], gathered.at[k, seat, :, lanes_of(mine, half)],
            x_send.at[k, i, h], x_recv.at[k, i, h], device(i, 0, h, 0),
        )

    def y_copy(k, i, side):
        at = (x - i + nx) % nx
        ref = gathered.at[k, pl.ds(2 * at, 2), :, lanes_of(2 * mine + side, quarter)]
        to = device(0, 0, 0, 2 * side - 1)
        return remote(ref, ref, y_send.at[k, i, side], y_recv.at[k, i, side], to)

    def ry_copy(k, side):
        to = device(0, 0, 0, 2 * side - 1)
        return remote(
            other.at[k, side], from_y.at[k, side], ry_send.at[k, side], ry_recv.at[k, side], to
        )

    def rx_copy(k, i, h):
        to = 2 * ((x - i + nx) % nx) + (c + h) % 2
        return remote(
            summed.at[k, to], back.at[k, seat],
            rx_send.at[k, i, h], rx_recv.at[k, i, h], device(-i, 0, h, 0),
        )

    z_copy(0, 1).start()
    z_copy(1, 1).start()
    for load in loads:
        load.wait()

    def spread(k):
        def step(j, carry):
            d = (k * per) // 2 + 1 + j
            z_copy(0, d).wait_recv()
            pl.when(d < reach)(lambda: z_copy(0, d + 1).start())

            @pl.when(d < reach)
            def _():
                z_copy(1, d).wait_recv()
                pl.when(d < reach - 1)(lambda: z_copy(1, d + 1).start())

            return carry

        lax.fori_loop(0, per // 2, step, 0)
        places = [place(k * per + i) for i in range(per)]
        got = jnp.concatenate([block[at, :, :half] for at in places], axis=0)
        table = jnp.concatenate([block[at, :, half:] for at in places], axis=0)
        share = jnp.dot(table, chosen_by, preferred_element_type=jnp.float32)
        named = share > 0.0
        rank = jnp.dot(
            before, jnp.where(named, 1.0, 0.0).astype(jnp.bfloat16),
            preferred_element_type=jnp.float32,
        )
        hit = in_block & named & (rank == slot_rank)
        lift[k] = jnp.where(hit, share, 0.0).astype(jnp.bfloat16)
        take = jnp.where(hit, 1.0, 0.0).T.astype(jnp.bfloat16)
        value = jnp.dot(take, got, preferred_element_type=jnp.float32)
        sent[k] = value.astype(jnp.bfloat16).reshape(2 * nx, tall, half)
        for i, h in others:
            x_copy(k, i, h).start()
        gathered[k, seat, :, lanes_of(mine, half)] = sent[k, seat]

    def relay(k):
        for i in range(nx):
            for h in range(2):
                if i or h:
                    x_copy(k, i, h).wait_recv()
            for side in range(2):
                y_copy(k, i, side).start()

    def compute(k):
        for i in range(nx):
            for side in range(2):
                y_copy(k, i, side).wait_recv()
        value = gathered[k].reshape(wide, width)
        gate = jnp.dot(value, w_gate[...], preferred_element_type=jnp.float32)
        upper = jnp.dot(value, w_up[...], preferred_element_type=jnp.float32)
        hidden = (gate / (1.0 + jnp.exp(-gate)) * upper).astype(jnp.bfloat16)

        def down(part):
            value = jnp.dot(
                hidden, w_down[:, lanes_of(part, quarter)], preferred_element_type=jnp.float32
            )
            return value.reshape(2 * nx, tall, quarter)

        for side in range(2):
            other[k, side] = down(2 * (1 - mine) + side).astype(jnp.bfloat16)
            ry_copy(k, side).start()
        for side in range(2):
            own[k, side] = down(2 * mine + side)

    def reduce(k):
        for side in range(2):
            ry_copy(k, side).wait_recv()
            summed[k, :, :, side * quarter : (side + 1) * quarter] = (
                own[k, side] + from_y[k, side].astype(jnp.float32)
            ).astype(jnp.bfloat16)
        for i, h in others:
            rx_copy(k, i, h).start()
        back[k, seat] = summed[k, seat]

    def combine(k):
        for i, h in others:
            rx_copy(k, i, h).wait_recv()
        value = jnp.dot(
            lift[k], back[k].reshape(wide, half), preferred_element_type=jnp.float32
        )
        local[pl.ds(k * per, per)] = value.reshape(per, rows, half)

    stages = (spread, relay, compute, reduce, combine)

    def tick(t, carry):
        for lag, stage in enumerate(stages):
            pl.when((t >= lag) & (t - lag < groups))(functools.partial(stage, t - lag))
        return carry

    lax.fori_loop(0, groups + len(stages) - 1, tick, 0)

    def rz_copy(way, d):
        to = device(0, 1 if way == 0 else -1, 0, 0)
        return remote(
            line_out.at[way, d], line_in.at[way, d], rz_send.at[way, d], rz_recv.at[way, d], to
        )

    farthest = (reach - 1, reach)

    def homeward(way, d):
        value = local[2 * d if way == 0 else 2 * d - 1]
        if d < farthest[way]:
            rz_copy(way, d + 1).wait_recv()
            value = value + line_in[way, d + 1].astype(jnp.float32)
        line_out[way, d] = value.astype(jnp.bfloat16)
        rz_copy(way, d).start()

    for d in range(reach, 0, -1):
        for way in (1, 0):
            if d <= farthest[way]:
                homeward(way, d)
    value = local[0]
    for way in range(2):
        rz_copy(way, 1).wait_recv()
        value = value + line_in[way, 1].astype(jnp.float32)
    last_out[...] = value.reshape(4, rows // 4, half)

    def last_copy(j):
        return remote(
            last_out.at[(y + j) % 4], last_in.at[y], last_send.at[j], last_recv.at[j],
            device(0, 0, 0, j),
        )

    for j in (2, 1, 3):
        last_copy(j).start()
    last_in[y] = last_out[y]
    for j in (1, 3, 2):
        last_copy(j).wait_recv()
    for side in range(2):
        out_ref[:, side * half : (side + 1) * half] = (
            last_in[side] + last_in[side + 2]
        ).astype(out_ref.dtype)

    for d in range(1, reach + 1):
        for way in range(2):
            if d <= (reach, reach - 1)[way]:
                z_copy(way, d).wait_send()
            if d <= farthest[way]:
                rz_copy(way, d).wait_send()
    for j in (1, 2, 3):
        last_copy(j).wait_send()

    def drain(k, carry):
        for i, h in others:
            x_copy(k, i, h).wait_send()
            rx_copy(k, i, h).wait_send()
        for side in range(2):
            for i in range(nx):
                y_copy(k, i, side).wait_send()
            ry_copy(k, side).wait_send()
        return carry

    lax.fori_loop(0, groups, drain, 0)


def by_exchange(tokens, expert_ids, route_logits, expert_gate, expert_up, expert_down):
    rows, width = tokens.shape
    hidden = expert_gate.shape[2]
    nx = 4
    nz = lax.axis_size("ep") // (2 * nx)
    per = 4
    groups, tall, reach = nz // per, per * SLOTS, nz // 2
    wide = 2 * nx * tall
    half, quarter, sub = width // 2, width // 4, rows // 4
    vmem = pl.BlockSpec(memory_space=pltpu.VMEM)
    anywhere = pl.BlockSpec(memory_space=pl.ANY)
    bf16, f32, dma = jnp.bfloat16, jnp.float32, pltpu.SemaphoreType.DMA
    return pl.pallas_call(
        functools.partial(exchange_kernel, nx, nz, per),
        out_shape=jax.ShapeDtypeStruct((sub, width), bf16),
        in_specs=[vmem, vmem, vmem, anywhere, anywhere, anywhere],
        out_specs=vmem,
        scratch_shapes=[
            pltpu.VMEM((width, hidden), bf16),
            pltpu.VMEM((width, hidden), bf16),
            pltpu.VMEM((hidden, width), bf16),
            pltpu.VMEM((nz, rows, half + LANES), bf16),
            pltpu.VMEM((groups, per * rows, wide), bf16),
            pltpu.VMEM((groups, 2 * nx, tall, half), bf16),
            pltpu.VMEM((groups, 2 * nx, tall, width), bf16),
            pltpu.VMEM((groups, 2, 2 * nx, tall, quarter), f32),
            pltpu.VMEM((groups, 2, 2 * nx, tall, quarter), bf16),
            pltpu.VMEM((groups, 2, 2 * nx, tall, quarter), bf16),
            pltpu.VMEM((groups, 2 * nx, tall, half), bf16),
            pltpu.VMEM((groups, 2 * nx, tall, half), bf16),
            pltpu.VMEM((nz, rows, half), f32),
            pltpu.VMEM((2, reach + 1, rows, half), bf16),
            pltpu.VMEM((2, reach + 1, rows, half), bf16),
            pltpu.VMEM((4, sub, half), f32),
            pltpu.VMEM((4, sub, half), f32),
            dma((3,)),
            dma((2, reach + 1)),
            dma((2, reach + 1)),
            dma((groups, nx, 2)),
            dma((groups, nx, 2)),
            dma((groups, nx, 2)),
            dma((groups, nx, 2)),
            dma((groups, 2)),
            dma((groups, 2)),
            dma((groups, nx, 2)),
            dma((groups, nx, 2)),
            dma((2, reach + 1)),
            dma((2, reach + 1)),
            dma((4,)),
            dma((4,)),
        ],
        compiler_params=pltpu.CompilerParams(
            collective_id=0, has_side_effects=True, vmem_limit_bytes=56 * 1024 * 1024
        ),
    )(tokens, expert_ids, route_logits, expert_gate, expert_up, expert_down)


def on_device(tokens, expert_ids, route_logits, expert_gate, expert_up, expert_down):
    rows, width = tokens.shape
    n_ep, n_dp = lax.axis_size("ep"), lax.axis_size("dp")
    fits = n_dp == 4 and n_ep == LANES and rows == 16 and width % 512 == 0
    fits = fits and expert_gate.shape[0] == 1 and expert_gate.shape[2] % LANES == 0
    run = by_exchange if fits else by_slots
    return run(tokens, expert_ids, route_logits, expert_gate, expert_up, expert_down)


def solution(mesh):
    placed = (
        P("ep", None),
        P("ep", None),
        P("ep", None),
        P("ep", None, "dp"),
        P("ep", None, "dp"),
        P("ep", "dp", None),
    )
    return jax.shard_map(
        on_device, mesh=mesh, in_specs=placed, out_specs=P(("ep", "dp"), None), check_vma=False
    )
```
